32 devices in a mesh: pq: 2 (over x), rs: 16 (over z, y, core).
Axes of the slice: x: 2, y: 2, z: 4, core: 2. Of those that a mesh axis runs over, the one named last changes fastest.
Arguments:
- integrals: bfloat16 [128, 1152, 1152], P('pq', 'rs'), may hold values from -6 to 6
- coeff: bfloat16 [1152, 896], P('rs', 'pq'), may hold values from -0.1875 to 0.1875
Outputs:
- half_mo: bfloat16 [128, 896, 896], P('pq', 'rs')
The draws below stay inside these ranges and needn't reach their ends.
All inputs are finite; a program needn't handle non-finite values.
Results may differ from the reference program's by a relative error of at most 0.0049.
Values may be sent and summed in bfloat16 or wider, within the bound.
A program may use at most 128 MiB of HBM per device.

```python
import jax
import jax.numpy as jnp
from jax import lax

NBASIS = 1152
NORB = 896
PAIRS = 128


def block_scale(own_key, dims, split, smallest, top_value):
    factor_of, own = 1.0, jax.random.fold_in(own_key, 6)
    for dim, parts in split:
        steps = jnp.exp(jax.random.uniform(jax.random.fold_in(own, dim), (parts,), jnp.float32, smallest / len(split), top_value / len(split)))
        factor_of = factor_of * jnp.repeat(steps, dims[dim] // parts).reshape([-1 if axis == dim else 1 for axis in range(len(dims))])
    return factor_of


def noise(own_key, shape, width, bound, cuts=(), kind=jnp.bfloat16):
    drawn = width * jax.random.normal(own_key, shape, jnp.float32)
    if cuts:
        drawn = drawn * block_scale(own_key, shape, cuts, -0.22, 0.18)
    return jnp.clip(drawn, -bound, bound).astype(kind)


def setup_inputs(seed: int = 0) -> dict:
    splits = jax.random.split(jax.random.key(seed), 3)
    return {
        "integrals": noise(splits[0], (PAIRS, NBASIS, NBASIS), 1.0, 6.0, ((0, 2), (1, 16))),
        "coeff": noise(splits[1], (NBASIS, NORB), NBASIS ** -0.5, 0.1875, ((0, 16), (1, 2))),
    }


def reference(integrals, coeff):
    pairs = integrals.shape[0]
    flat = integrals.reshape(pairs * NBASIS, NBASIS)
    first = jnp.dot(flat, coeff, preferred_element_type=jnp.float32).astype(jnp.bfloat16)
    first = first.reshape(pairs, NBASIS, NORB)

    def one_row(block):
        return jnp.dot(block.T, coeff, preferred_element_type=jnp.float32).astype(jnp.bfloat16)

    return lax.map(one_row, first)
```

```python
import functools
import math

import jax
import jax.numpy as jnp
from jax import lax
from jax.experimental import pallas as pl
from jax.experimental.pallas import tpu as pltpu
from jax.sharding import PartitionSpec as P

MESH = pl.DeviceIdType.MESH


def second_half(received, panel):
    return jnp.einsum("prl,rk->plk", received, panel, preferred_element_type=jnp.float32).astype(
        jnp.bfloat16
    )


def plain(integrals, panel):
    pair_rows, block_rows, nbasis = integrals.shape
    flat = integrals.reshape(pair_rows * block_rows, nbasis)
    first = jnp.dot(flat, panel, preferred_element_type=jnp.float32).astype(jnp.bfloat16)
    first = first.reshape(pair_rows, block_rows, panel.shape[1])
    return second_half(lax.all_to_all(first, "rs", split_axis=2, concat_axis=1, tiled=True), panel)


def fused_kernel(n, group, x_ref, c_ref, o_ref, tiles, parts, panel, send, recv, load_sem, send_sem, recv_sem, own_sem, hop_sem, part_sem):
    me = lax.axis_index("rs")
    col = lax.axis_index("pq")
    groups = send.shape[0]
    rows = send.shape[2]
    width = send.shape[3] // group
    nbasis = tiles.shape[3]
    half = n // 2
    far_side = lax.rem(me // half + 1, 2)
    near_side = me // half
    far = far_side * half
    near = near_side * half
    lines = n // 4
    core = lax.rem(me, 2)
    y = lax.rem(me // 2, 2)
    z = me // 4
    col_too = 1 - col
    columns = c_ref.shape[1]
    lead = 128
    leaders = lead // width

    def spot(at_z, at_y, at_core):
        return at_z * 4 + at_y * 2 + at_core

    def load(g):
        return pltpu.make_async_copy(x_ref.at[pl.ds(g * group, group)], tiles.at[g % 2], load_sem.at[g % 2])


    def far_partner(i):
        pair = lax.rem(lax.div(lax.rem(me, half), 2) + (i // 2 if isinstance(i, int) else lax.div(i, 2)), half // 2)
        return far + pair * 2 + lax.rem(me + i, 2)

    def partner(i):
        if not isinstance(i, int) or i < half:
            return far_partner(i)
        return near + lax.rem(me + i - half + 1, half)

    cuts = 3 if rows % 24 == 0 else 1
    short = rows // cuts

    def remote(g, i, at=0, count=rows):
        to = partner(i)
        return pltpu.make_async_remote_copy(
            src_ref=send.at[g, to, pl.ds(at, count)],
            dst_ref=recv.at[g, me, pl.ds(at, count)],
            send_sem=send_sem.at[g, i],
            recv_sem=recv_sem.at[g, i],
            device_id={"rs": to},
            device_id_type=MESH,
        )

    def own(g):
        return pltpu.make_async_copy(send.at[g, me], recv.at[g, me], own_sem.at[g])

    load(0).start()
    load(1).start()
    parts[col, me] = c_ref[...]
    barrier = pltpu.get_barrier_semaphore()
    for i in range(1, n):
        pl.semaphore_signal(barrier, inc=1, device_id={"rs": lax.rem(me + i, n)}, device_id_type=MESH)
    across_y = {"rs": spot(z, 1 - y, core)}
    across_x = {"pq": col_too}
    diagonal = {"pq": col_too, "rs": spot(z, 1 - y, core)}
    across_core = {"rs": spot(z, y, 1 - core)}
    for to in (across_x, diagonal):
        pl.semaphore_signal(barrier, inc=1, device_id=to, device_id_type=MESH)
    pl.semaphore_wait(barrier, n + 1)

    hops = []
    lanes = (pl.ds(0, lead), pl.ds(lead, columns - lead))

    def hop(s, q, r, to, sem):
        return pltpu.make_async_remote_copy(
            src_ref=parts.at[q, r, :, lanes[s]],
            dst_ref=parts.at[q, r, :, lanes[s]],
            send_sem=hop_sem.at[sem],
            recv_sem=part_sem.at[s, q, r],
            device_id=to,
            device_id_type=MESH,
        )

    def pass_on(s, q, r, *targets):
        for to in targets:
            copy = hop(s, q, r, to, len(hops))
            copy.start()
            hops.append(copy)

    def arrived(s, q, r):
        hop(s, q, r, across_x, 0).wait_recv()

    def along(k):
        return lax.rem(z + lines - k, lines)

    def arrived_from_core(s, q):
        for k in range(lines):
            for at_y in (0, 1):
                arrived(s, q, spot(k, at_y, 1 - core))

    for k in range(1, lines):
        pass_on(0, col, me, {"rs": spot(lax.rem(z + k, lines), y, core)})
    for k in range(lines):
        r = spot(along(k), y, core)
        if k:
            arrived(0, col, r)
        pass_on(0, col, r, across_y, across_x, diagonal, across_core)
    deep = lines // 2
    z_base = lax.div(z, deep) * deep
    opposite = lax.rem(z + deep, lines)
    o_base = lax.div(opposite, deep) * deep
    mates = [z_base + lax.rem(z + k, deep) for k in range(1, deep)]
    others = [o_base + lax.rem(z + k, deep) for k in range(1, deep)]
    pass_on(1, col, me, {"rs": spot(opposite, y, core)}, *({"rs": spot(m, y, core)} for m in mates))
    pass_on(1, col, me, across_y, across_x, across_core)
    for k in range(lines):
        mine, other = spot(along(k), y, core), spot(along(k), 1 - y, core)
        for q, r in ((col, other), (col_too, mine), (col_too, other)):
            arrived(0, q, r)
            pass_on(0, q, r, across_core)

    def weights(side, at, count):
        q = near_side if side else far_side
        return parts[q, :, :, at : at + count].reshape(nbasis, count)

    def ahead(g, cuts):
        load(g).wait()
        first_i = 2 * lax.rem(half // 2 - lax.div(lax.rem(me, half), 2), half // 2)
        count = rows // cuts
        for cut in range(cuts):
            block = tiles[g % 2, :, cut * count : (cut + 1) * count].reshape(group * count, nbasis)
            first = jnp.dot(block, weights(0, 0, lead), preferred_element_type=jnp.float32)
            for slot in range(group):
                piece = first[slot * count : (slot + 1) * count].astype(jnp.bfloat16)
                for d in range(-(-lead // width)):
                    end = min((d + 1) * width, lead)
                    send[g, far + d, cut * count : (cut + 1) * count, slot * width : slot * width + end - d * width] = piece[:, d * width : end]
            for j in range(leaders):
                remote(g, first_i + j, cut * count, count).start()

    def behind(g):
        first_i = 2 * lax.rem(half // 2 - lax.div(lax.rem(me, half), 2), half // 2)
        for q in range(group // step):
            block = tiles[g % 2, q * step : (q + 1) * step].reshape(step * rows, nbasis)
            first = jnp.dot(block, weights(0, lead, columns - lead), preferred_element_type=jnp.float32)
            for j in range(step):
                slot = q * step + j
                piece = first[j * rows : (j + 1) * rows].astype(jnp.bfloat16)
                for d in range(leaders, half):
                    start = max(d * width, lead)
                    send[g, far + d, :, slot * width + start - d * width : (slot + 1) * width] = piece[:, start - lead : (d + 1) * width - lead]
        for j in range(leaders, half):
            remote(g, lax.rem(first_i + j, half)).start()

    step = 4
    early = 2
    arrived_from_core(0, far_side)
    ahead(0, cuts)
    line = [z, *mates, opposite, *others]
    for k in range(1, lines):
        r = spot(line[k], y, core)
        arrived(1, col, r)
        if k == deep:
            pass_on(1, col, r, *({"rs": spot(m, y, core)} for m in mates))
        pass_on(1, col, r, across_y, across_x, across_core)
    ahead(1, 1)
    for k in range(lines):
        mine, other = spot(line[k], y, core), spot(line[k], 1 - y, core)
        arrived(1, col_too, mine)
        arrived(1, col, other)
        if k % 2:
            pass_on(1, col, other, across_x)
        else:
            pass_on(1, col_too, mine, across_y)
        pass_on(1, col_too, mine, across_core)
        pass_on(1, col, other, across_core)
    for k in range(lines):
        other = spot(line[k], 1 - y, core)
        arrived(1, col_too, other)
        pass_on(1, col_too, other, across_core)
    arrived_from_core(1, far_side)

    for g in range(groups):
        if 0 < g < groups - 1:
            load(g + 1).start()
        if g >= early:
            load(g).wait()
        for side in (0, 1):
            if side == 0 and g < early:
                behind(g)
                continue
            if g == 0:
                arrived_from_core(0, near_side)
                arrived_from_core(1, near_side)
            base = near if side else far
            for q in range(group // step):
                block = tiles[g % 2, q * step : (q + 1) * step].reshape(step * rows, nbasis)
                first = jnp.dot(block, weights(side, 0, columns), preferred_element_type=jnp.float32)
                for j in range(step):
                    slot = q * step + j
                    piece = first[j * rows : (j + 1) * rows].astype(jnp.bfloat16)
                    for d in range(half):
                        send[g, base + d, :, slot * width : (slot + 1) * width] = piece[:, d * width : (d + 1) * width]
            for i in range(half, n - 1) if side else range(half):
                remote(g, i).start()
        own(g).start()

    for q in (0, 1):
        panel[:, q * half * width : (q + 1) * half * width] = parts[q].reshape(nbasis, half * width)
    for copy in hops:
        copy.wait_send()

    contract = (((0,), (0,)), ((), ()))
    for g in range(groups):
        own(g).wait()
        if g + 1 < groups:
            for i in range(n - 1):
                remote(g, i).wait()
            lhs = recv[g].reshape(n * rows, group * width)
            out = lax.dot_general(lhs, panel[...], contract, preferred_element_type=jnp.float32)
        else:
            for i in range(half, n - 1):
                remote(g, i).wait()
            chunks = [(near, half)]
            for a in range(half // 2):
                pair = lax.rem(lax.rem(me, half) // 2 + half // 2 - a, half // 2)
                chunks.append((far + 2 * pair, 2))
            out = 0.0
            for at, (base, count) in enumerate(chunks):
                if at:
                    remote(g, 2 * at - 2).wait()
                    remote(g, 2 * at - 1).wait()
                lhs = recv[g, pl.ds(base, count)].reshape(count * rows, group * width)
                part = panel[pl.ds(pl.multiple_of(base * rows, 16), count * rows)]
                out += lax.dot_general(lhs, part, contract, preferred_element_type=jnp.float32)
        for j in range(group):
            o_ref[g * group + j] = out[j * width : (j + 1) * width].astype(jnp.bfloat16)


def fused(n, group, integrals, coeff):
    pair_rows, rows, nbasis = integrals.shape
    columns = coeff.shape[1]
    norb = 2 * columns
    width = norb // n
    groups = pair_rows // group
    flops = 2 * pair_rows * rows * nbasis * norb + 2 * pair_rows * width * n * rows * norb
    sent = 2 * pair_rows * rows * norb
    return pl.pallas_call(
        functools.partial(fused_kernel, n, group),
        out_shape=pltpu.VMEM((pair_rows, width, norb), jnp.bfloat16),
        in_specs=[pl.BlockSpec(memory_space=pl.ANY), pl.BlockSpec(memory_space=pltpu.VMEM)],
        out_specs=pl.BlockSpec(memory_space=pltpu.VMEM),
        scratch_shapes=[
            pltpu.VMEM((2, group, rows, nbasis), jnp.bfloat16),
            pltpu.VMEM((2, n, rows, columns), jnp.bfloat16),
            pltpu.VMEM((nbasis, norb), jnp.bfloat16),
            pltpu.VMEM((groups, n, rows, group * width), jnp.bfloat16),
            pltpu.VMEM((groups, n, rows, group * width), jnp.bfloat16),
            pltpu.SemaphoreType.DMA((2,)),
            pltpu.SemaphoreType.DMA((groups, n)),
            pltpu.SemaphoreType.DMA((groups, n)),
            pltpu.SemaphoreType.DMA((groups,)),
            pltpu.SemaphoreType.DMA((5 * n,)),
            pltpu.SemaphoreType.DMA((2, 2, n)),
        ],
        compiler_params=pltpu.CompilerParams(
            collective_id=0, has_side_effects=True, vmem_limit_bytes=50 * 2**20
        ),
        cost_estimate=pl.CostEstimate(flops=flops, bytes_accessed=4 * sent, transcendentals=0),
    )(integrals, coeff)


def on_device(n, splits, integrals, coeff):
    pair_rows, rows, nbasis = integrals.shape
    columns = coeff.shape[1]
    norb = columns * splits
    width = norb // n
    group = math.lcm(4, 128 // math.gcd(width, 128))
    aligned = rows % 8 == 0 and width % 8 == 0 and pair_rows % group == 0 and pair_rows >= 2 * group
    if splits == 2 and n % 8 == 0 and aligned and group * width <= 2048 and 2 * width <= 128 < columns:
        return fused(n, group, integrals, coeff)
    strip = lax.all_gather(coeff, "pq", axis=1, tiled=True)
    return plain(integrals, lax.all_gather(strip, "rs", axis=0, tiled=True))


def solution(mesh):
    placed = (P("pq", "rs", None), P("rs", "pq"))
    return jax.shard_map(
        functools.partial(on_device, mesh.shape["rs"], mesh.shape["pq"]),
        mesh=mesh,
        in_specs=placed,
        out_specs=P("pq", "rs", None),
        check_vma=False,
    )
```

```python
import functools
import math

import jax
import jax.numpy as jnp
from jax import lax
from jax.experimental import pallas as pl
from jax.experimental.pallas import tpu as pltpu
from jax.sharding import PartitionSpec as P

MESH = pl.DeviceIdType.MESH


def second_half(received, panel):
    return jnp.einsum("prl,rk->plk", received, panel, preferred_element_type=jnp.float32).astype(
        jnp.bfloat16
    )


def plain(integrals, panel):
    pair_rows, block_rows, nbasis = integrals.shape
    flat = integrals.reshape(pair_rows * block_rows, nbasis)
    first = jnp.dot(flat, panel, preferred_element_type=jnp.float32).astype(jnp.bfloat16)
    first = first.reshape(pair_rows, block_rows, panel.shape[1])
    return second_half(lax.all_to_all(first, "rs", split_axis=2, concat_axis=1, tiled=True), panel)


def fused_kernel(n, group, x_ref, c_ref, o_ref, tiles, parts, panel, send, recv, load_sem, send_sem, recv_sem, own_sem, hop_sem, part_sem, local_sem):
    me = lax.axis_index("rs")
    col = lax.axis_index("pq")
    groups = send.shape[0]
    rows = send.shape[2]
    width = send.shape[3] // group
    nbasis = tiles.shape[3]
    half = n // 2
    far_side = lax.rem(me // half + 1, 2)
    near_side = me // half
    far = far_side * half
    near = near_side * half
    lines = n // 4
    core = lax.rem(me, 2)
    y = lax.rem(me // 2, 2)
    z = me // 4
    col_too = 1 - col
    columns = c_ref.shape[1]
    lead = 128
    leaders = lead // width

    def spot(at_z, at_y, at_core):
        return at_z * 4 + at_y * 2 + at_core

    def load(g):
        return pltpu.make_async_copy(x_ref.at[pl.ds(g * group, group)], tiles.at[g % 2], load_sem.at[g % 2])


    def far_partner(i):
        pair = lax.rem(lax.div(lax.rem(me, half), 2) + (i // 2 if isinstance(i, int) else lax.div(i, 2)), half // 2)
        return far + pair * 2 + lax.rem(me + i, 2)

    def partner(i):
        if not isinstance(i, int) or i < half:
            return far_partner(i)
        return near + lax.rem(me + i - half + 1, half)

    def remote(g, i, at=0, count=rows):
        to = partner(i)
        return pltpu.make_async_remote_copy(
            src_ref=send.at[g, to, pl.ds(at, count)],
            dst_ref=recv.at[g, me, pl.ds(at, count)],
            send_sem=send_sem.at[g, i],
            recv_sem=recv_sem.at[g, i],
            device_id={"rs": to},
            device_id_type=MESH,
        )

    def own(g):
        return pltpu.make_async_copy(send.at[g, me], recv.at[g, me], own_sem.at[g])

    local = pltpu.make_async_copy(c_ref, parts.at[col, me], local_sem)
    local.start()
    barrier = pltpu.get_barrier_semaphore()
    for i in range(1, n):
        pl.semaphore_signal(barrier, inc=1, device_id={"rs": lax.rem(me + i, n)}, device_id_type=MESH)
    across_y = {"rs": spot(z, 1 - y, core)}
    across_x = {"pq": col_too}
    diagonal = {"pq": col_too, "rs": spot(z, 1 - y, core)}
    across_core = {"rs": spot(z, y, 1 - core)}
    for to in (across_x, diagonal):
        pl.semaphore_signal(barrier, inc=1, device_id=to, device_id_type=MESH)
    load(0).start()
    load(1).start()
    local.wait()
    pl.semaphore_wait(barrier, n + 1)

    hops = []
    lanes = (pl.ds(0, lead), pl.ds(lead, columns - lead))

    def hop(s, q, r, to, sem):
        return pltpu.make_async_remote_copy(
            src_ref=parts.at[q, r, :, lanes[s]],
            dst_ref=parts.at[q, r, :, lanes[s]],
            send_sem=hop_sem.at[sem],
            recv_sem=part_sem.at[s, q, r],
            device_id=to,
            device_id_type=MESH,
        )

    def pass_on(s, q, r, *targets):
        for to in targets:
            copy = hop(s, q, r, to, len(hops))
            copy.start()
            hops.append(copy)

    def arrived(s, q, r):
        hop(s, q, r, across_x, 0).wait_recv()

    def along(k):
        return lax.rem(z + lines - k, lines)

    def arrived_from_core(s, q):
        for k in range(lines):
            for at_y in (0, 1):
                arrived(s, q, spot(k, at_y, 1 - core))

    for k in range(1, lines):
        pass_on(0, col, me, {"rs": spot(lax.rem(z + k, lines), y, core)})
    for k in range(lines):
        r = spot(along(k), y, core)
        if k:
            arrived(0, col, r)
        pass_on(0, col, r, across_y, across_x, diagonal, across_core)
    deep = lines // 2
    z_base = lax.div(z, deep) * deep
    opposite = lax.rem(z + deep, lines)
    o_base = lax.div(opposite, deep) * deep
    mates = [z_base + lax.rem(z + k, deep) for k in range(1, deep)]
    others = [o_base + lax.rem(z + k, deep) for k in range(1, deep)]
    pass_on(1, col, me, {"rs": spot(opposite, y, core)}, *({"rs": spot(m, y, core)} for m in mates))
    pass_on(1, col, me, across_y, across_x, across_core)
    for k in range(lines):
        mine, other = spot(along(k), y, core), spot(along(k), 1 - y, core)
        for q, r in ((col, other), (col_too, mine), (col_too, other)):
            arrived(0, q, r)
            pass_on(0, q, r, across_core)

    def weights(side, at, count):
        q = near_side if side else far_side
        return parts[q, :, :, at : at + count].reshape(nbasis, count)

    def ahead(g, cuts):
        load(g).wait()
        first_i = 2 * lax.rem(half // 2 - lax.div(lax.rem(me, half), 2), half // 2)
        for at, count in cuts:
            block = tiles[g % 2, :, at : at + count].reshape(group * count, nbasis)
            first = jnp.dot(block, weights(0, 0, lead), preferred_element_type=jnp.float32)
            for slot in range(group):
                piece = first[slot * count : (slot + 1) * count].astype(jnp.bfloat16)
                for d in range(-(-lead // width)):
                    end = min((d + 1) * width, lead)
                    send[g, far + d, at : at + count, slot * width : slot * width + end - d * width] = piece[:, d * width : end]
            for j in range(leaders):
                remote(g, first_i + j, at, count).start()

    def behind(g):
        first_i = 2 * lax.rem(half // 2 - lax.div(lax.rem(me, half), 2), half // 2)
        for q in range(group // step):
            block = tiles[g % 2, q * step : (q + 1) * step].reshape(step * rows, nbasis)
            first = jnp.dot(block, weights(0, lead, columns - lead), preferred_element_type=jnp.float32)
            for j in range(step):
                slot = q * step + j
                piece = first[j * rows : (j + 1) * rows].astype(jnp.bfloat16)
                for d in range(leaders, half):
                    start = max(d * width, lead)
                    send[g, far + d, :, slot * width + start - d * width : (slot + 1) * width] = piece[:, start - lead : (d + 1) * width - lead]
        for idx in range(half - leaders):
            remote(g, idx + leaders * (idx >= first_i).astype(jnp.int32)).start()

    step = 4
    early = 2
    arrived_from_core(0, far_side)
    ahead(0, ((0, 8), (8, 24), (32, rows - 32)) if rows > 32 else ((0, rows),))
    line = [z, *mates, opposite, *others]
    for k in range(1, lines):
        r = spot(line[k], y, core)
        arrived(1, col, r)
        if k == deep:
            pass_on(1, col, r, *({"rs": spot(m, y, core)} for m in mates))
        pass_on(1, col, r, across_y, across_x, across_core)
    ahead(1, ((0, rows),))
    for k in range(lines):
        mine, other = spot(line[k], y, core), spot(line[k], 1 - y, core)
        arrived(1, col_too, mine)
        arrived(1, col, other)
        if k % 2:
            pass_on(1, col, other, across_x)
        else:
            pass_on(1, col_too, mine, across_y)
        pass_on(1, col_too, mine, across_core)
        pass_on(1, col, other, across_core)
    for k in range(lines):
        other = spot(line[k], 1 - y, core)
        arrived(1, col_too, other)
        pass_on(1, col_too, other, across_core)
    arrived_from_core(1, far_side)

    for g in range(groups):
        if 0 < g < groups - 1:
            load(g + 1).start()
        if g >= early:
            load(g).wait()
        for side in (0, 1) if g + 1 < groups else (1, 0):
            if side == 0 and g < early:
                behind(g)
                continue
            if g == 0:
                arrived_from_core(0, near_side)
                arrived_from_core(1, near_side)
            base = near if side else far
            for q in range(group // step):
                block = tiles[g % 2, q * step : (q + 1) * step].reshape(step * rows, nbasis)
                first = jnp.dot(block, weights(side, 0, columns), preferred_element_type=jnp.float32)
                for j in range(step):
                    slot = q * step + j
                    piece = first[j * rows : (j + 1) * rows].astype(jnp.bfloat16)
                    for d in range(half):
                        send[g, base + d, :, slot * width : (slot + 1) * width] = piece[:, d * width : (d + 1) * width]
            for i in range(half, n - 1) if side else range(half):
                remote(g, i).start()
        own(g).start()

    for q in (0, 1):
        panel[:, q * half * width : (q + 1) * half * width] = parts[q].reshape(nbasis, half * width)
    for copy in hops:
        copy.wait_send()

    contract = (((0,), (0,)), ((), ()))
    for g in range(groups):
        own(g).wait()
        if g + 1 < groups:
            for i in range(n - 1):
                remote(g, i).wait()
            lhs = recv[g].reshape(n * rows, group * width)
            out = lax.dot_general(lhs, panel[...], contract, preferred_element_type=jnp.float32)
        else:
            for i in range(half, n - 1):
                remote(g, i).wait()
            chunks = [(near, half)]
            for a in range(half // 2):
                pair = lax.rem(lax.rem(me, half) // 2 + half // 2 - a, half // 2)
                chunks.append((far + 2 * pair, 2))
            out = 0.0
            for at, (base, count) in enumerate(chunks):
                if at:
                    remote(g, 2 * at - 2).wait()
                    remote(g, 2 * at - 1).wait()
                lhs = recv[g, pl.ds(base, count)].reshape(count * rows, group * width)
                part = panel[pl.ds(pl.multiple_of(base * rows, 16), count * rows)]
                out += lax.dot_general(lhs, part, contract, preferred_element_type=jnp.float32)
        for j in range(group):
            o_ref[g * group + j] = out[j * width : (j + 1) * width].astype(jnp.bfloat16)


def fused(n, group, integrals, coeff):
    pair_rows, rows, nbasis = integrals.shape
    columns = coeff.shape[1]
    norb = 2 * columns
    width = norb // n
    groups = pair_rows // group
    flops = 2 * pair_rows * rows * nbasis * norb + 2 * pair_rows * width * n * rows * norb
    sent = 2 * pair_rows * rows * norb
    return pl.pallas_call(
        functools.partial(fused_kernel, n, group),
        out_shape=pltpu.VMEM((pair_rows, width, norb), jnp.bfloat16),
        in_specs=[pl.BlockSpec(memory_space=pl.ANY), pl.BlockSpec(memory_space=pl.ANY)],
        out_specs=pl.BlockSpec(memory_space=pltpu.VMEM),
        scratch_shapes=[
            pltpu.VMEM((2, group, rows, nbasis), jnp.bfloat16),
            pltpu.VMEM((2, n, rows, columns), jnp.bfloat16),
            pltpu.VMEM((nbasis, norb), jnp.bfloat16),
            pltpu.VMEM((groups, n, rows, group * width), jnp.bfloat16),
            pltpu.VMEM((groups, n, rows, group * width), jnp.bfloat16),
            pltpu.SemaphoreType.DMA((2,)),
            pltpu.SemaphoreType.DMA((groups, n)),
            pltpu.SemaphoreType.DMA((groups, n)),
            pltpu.SemaphoreType.DMA((groups,)),
            pltpu.SemaphoreType.DMA((5 * n,)),
            pltpu.SemaphoreType.DMA((2, 2, n)),
            pltpu.SemaphoreType.DMA,
        ],
        compiler_params=pltpu.CompilerParams(
            collective_id=0, has_side_effects=True, vmem_limit_bytes=50 * 2**20
        ),
        cost_estimate=pl.CostEstimate(flops=flops, bytes_accessed=4 * sent, transcendentals=0),
    )(integrals, coeff)


def on_device(n, splits, integrals, coeff):
    pair_rows, rows, nbasis = integrals.shape
    columns = coeff.shape[1]
    norb = columns * splits
    width = norb // n
    group = math.lcm(4, 128 // math.gcd(width, 128))
    aligned = rows % 8 == 0 and width % 8 == 0 and pair_rows % group == 0 and pair_rows >= 2 * group
    if splits == 2 and n % 8 == 0 and aligned and group * width <= 2048 and 2 * width <= 128 < columns:
        return fused(n, group, integrals, coeff)
    strip = lax.all_gather(coeff, "pq", axis=1, tiled=True)
    return plain(integrals, lax.all_gather(strip, "rs", axis=0, tiled=True))


def solution(mesh):
    placed = (P("pq", "rs", None), P("rs", "pq"))
    return jax.shard_map(
        functools.partial(on_device, mesh.shape["rs"], mesh.shape["pq"]),
        mesh=mesh,
        in_specs=placed,
        out_specs=P("pq", "rs", None),
        check_vma=False,
    )
```
